512 devices in a mesh: cuts: 16 (over y, x_hi, core), grid: 32 (over z, x_lo).
Axes of the slice: x: 4 (x_hi: 2, x_lo: 2; x = x_hi * 2 + x_lo), y: 4, z: 16, core: 2. Of those that a mesh axis runs over, the one named last changes fastest.
Arguments:
- orbitals: bfloat16 [131072, 4096], P('grid', 'cuts'), may hold values from -9 to 9, as said below
- potential: float32 [131072], P('grid'), may hold values from -1 to 1
- core_density: float32 [131072], P('grid'), may hold values from 0.05 to 0.5
- occupation: int32 [4096], P('cuts'), may hold values from 0 to 2
- slice_counts: int32 [16], P('cuts'), may hold values from 128 to 256
Outputs:
- orbitals_out: bfloat16 [131072, 4096], P('grid', 'cuts')
- potential_out: float32 [131072], P('grid')
The draws below stay inside these ranges and needn't reach their ends.
Inputs may be any that keep to these rules, and one draw needn't show every extreme that they name: `orbitals`: every entry has magnitude at most 9.
All inputs are finite; a program needn't handle non-finite values.
Results may differ from the reference program's by a relative error of at most 0.0015.
The reference program's roundings to bfloat16 on the way (of `applied` and `rotation`) count: a program that leaves them out, or rounds other values in their place, can miss the bound.
Values may be sent and summed in bfloat16 or wider, within the bound.
No kernel may reach another device: no remote copies, remote signals or barrier semaphores. Data moves between devices by JAX's collectives and lax.ppermute only.
A program may use at most 64 MiB of HBM per device.

```python
import math
import jax
import jax.numpy as jnp
from jax import lax

SLICE = 256
STATES = 4096
NG = 131072
N_CUTS = 16


def draw_orbitals(key, part):
    noise = jnp.clip(jax.random.normal(key, (NG, STATES), jnp.float32), -6.0, 6.0)
    mixed = noise + 0.5 * jnp.roll(noise, 1, axis=1)
    return mixed.astype(jnp.bfloat16)


def with_ends(values, rng, smallest, high):
    longest = values.shape.index(max(values.shape))
    spots = []
    for shift in (0, 1):
        where = [jax.random.randint(jax.random.fold_in(rng, axis), (), 0, length) for axis, length in enumerate(values.shape)]
        where[longest] = (where[longest] + shift) % values.shape[longest]
        spots.append(tuple(where))
    return values.at[spots[0]].set(smallest).at[spots[1]].set(high)


def levels(own_key, extent, shards, smallest, high):
    gain, own = 1.0, jax.random.fold_in(own_key, 6)
    for dim, shards_of in shards:
        draws = jnp.exp(jax.random.uniform(jax.random.fold_in(own, dim), (shards_of,), jnp.float32, smallest / len(shards), high / len(shards)))
        gain = gain * jnp.repeat(draws, extent[dim] // shards_of).reshape([-1 if axis == dim else 1 for axis in range(len(extent))])
    return gain


def setup_inputs(seed: int = 0) -> dict:
    splits = jax.random.split(jax.random.key(seed), 6)
    orbitals = draw_orbitals(jax.random.fold_in(splits[5], 71), 0)
    potential = jnp.clip(jax.random.uniform(splits[1], (NG,), jnp.float32, -1.0, 1.0) * levels(splits[1], (NG,), ((0, 32),), -0.4, 0.0), -1.0, 1.0)
    core_density = jnp.clip(jnp.exp(math.log(0.5) - 2.3025851 * jax.random.uniform(splits[2], (NG,), jnp.float32) ** levels(splits[2], (NG,), ((0, 32),), -0.2, 0.2)), 0.05, 0.5)
    occupation = with_ends(jax.random.randint(splits[3], (STATES,), 0, 3), jax.random.fold_in(splits[3], 1), 0, 2).astype(jnp.int32)
    slice_counts = with_ends(jax.random.randint(splits[4], (N_CUTS,), SLICE // 2, SLICE + 1), jax.random.fold_in(splits[4], 1), SLICE // 2, SLICE).astype(jnp.int32)
    return {"orbitals": orbitals, "potential": potential, "core_density": core_density, "occupation": occupation, "slice_counts": slice_counts}


mixing = 0.3
step_size = 0.5

def reference(orbitals, potential, core_density, occupation, slice_counts):
    highest = lax.Precision.HIGHEST
    coefficient = (3.0 / jnp.pi) ** (1.0 / 3.0)
    density = core_density.astype(jnp.float32)
    blocks = []
    for group in range(N_CUTS):
        psi = orbitals[:, group * SLICE:(group + 1) * SLICE]
        wide = psi.astype(jnp.float32)
        kinetic = -0.5 * (jnp.roll(wide, -1, axis=0) + jnp.roll(wide, 1, axis=0) - 2.0 * wide)
        applied = (kinetic + potential[:, None] * wide).astype(jnp.bfloat16)
        intersection = jnp.dot(psi.T.astype(jnp.float32), psi.astype(jnp.float32), preferred_element_type=jnp.float32) / NG
        ritz = jnp.dot(psi.T.astype(jnp.float32), applied.astype(jnp.float32), preferred_element_type=jnp.float32) / NG
        factor = jnp.linalg.cholesky(intersection)
        identity = jnp.eye(SLICE, dtype=jnp.float32)
        inverse = lax.linalg.triangular_solve(factor, identity, left_side=True, lower=True)
        projected = jnp.dot(jnp.dot(inverse, ritz, precision=highest), inverse.T, precision=highest)
        rotation = jnp.dot(inverse.T, identity - step_size * projected, precision=highest).astype(jnp.bfloat16)
        rotated = jnp.dot(psi.astype(jnp.float32), rotation.astype(jnp.float32), preferred_element_type=jnp.float32)
        blocks.append(rotated.astype(jnp.bfloat16))
        live = (jnp.arange(SLICE) < slice_counts[group]).astype(jnp.float32)
        weights = occupation[group * SLICE:(group + 1) * SLICE].astype(jnp.float32) * live / (2.0 * STATES)
        density = density + jnp.sum(rotated * rotated * weights[None, :], axis=1)
    potential_out = (1.0 - mixing) * potential + mixing * (-coefficient * jnp.cbrt(density))
    return (jnp.concatenate(blocks, axis=1), potential_out)
```

```python
import jax
import jax.numpy as jnp
from jax import lax
from jax.experimental import pallas as pl
from jax.experimental.pallas import tpu as pltpu
from jax.sharding import Mesh
from jax.sharding import PartitionSpec as P

GRID = ("grid_0", "grid_1")
HIGHEST = lax.Precision.HIGHEST
F32 = jnp.float32
BF16 = jnp.bfloat16

mixing = 0.3
step_size = 0.5

PANEL = 64
CHUNK = 512
EDGE = 16


def row_dot(a, b, precision=None):
    return lax.dot_general(a, b, (((0,), (0,)), ((), ())), precision=precision, preferred_element_type=F32)


def gram_kernel(psi_ref, potential_ref, out_ref, psi_v, applied_v, sems):
    rows, width = psi_ref.shape
    n = rows // CHUNK
    copies = [
        pltpu.make_async_copy(
            psi_ref.at[pl.ds(c * CHUNK, CHUNK)], psi_v.at[pl.ds(EDGE + c * CHUNK, CHUNK)], sems.at[c]
        )
        for c in range(n)
    ]
    for copy in copies:
        copy.start()
    psi_v[0:EDGE] = jnp.zeros((EDGE, width), BF16)
    psi_v[EDGE + rows : EDGE + rows + EDGE] = jnp.zeros((EDGE, width), BF16)
    by_row = jnp.transpose(potential_ref[...])
    copies[0].wait()
    intersection = ritz = None
    for c in range(n):
        if c + 1 < n:
            copies[c + 1].wait()
        for s in range(CHUNK // 128):
            start = c * CHUNK + s * 128
            block = start // 128
            wide = psi_v[start : start + 128 + 2 * EDGE].astype(F32)
            length = wide.shape[0]
            after = pltpu.roll(wide, length - 1, 0)[EDGE : EDGE + 128]
            before = pltpu.roll(wide, 1, 0)[EDGE : EDGE + 128]
            middle = wide[EDGE : EDGE + 128]
            kinetic = -0.5 * (after + before - 2.0 * middle)
            applied_v[start : start + 128] = (kinetic + by_row[:, block : block + 1] * middle).astype(BF16)
        psi = psi_v[EDGE + c * CHUNK : EDGE + (c + 1) * CHUNK]
        applied = applied_v[c * CHUNK : (c + 1) * CHUNK]
        one, two = row_dot(psi, psi), row_dot(psi, applied)
        intersection = one if c == 0 else intersection + one
        ritz = two if c == 0 else ritz + two
    out_ref[:, :width] = intersection
    out_ref[:, width:] = ritz


def pack_kernel(gram_ref, last_ref, next_ref, out_ref):
    width = gram_ref.shape[0]
    zeros = jnp.zeros((14, width), F32)
    last, following = last_ref[...].astype(F32), next_ref[...].astype(F32)
    left = jnp.concatenate([last, following, zeros], axis=0).astype(BF16)
    right = jnp.concatenate([following, last, zeros], axis=0).astype(BF16)
    across = row_dot(left, right)
    for i in range(width // 8):
        diagonal = jnp.zeros((1, 128), F32)
        for h in range(width // 128):
            intersection = gram_ref[8 * i : 8 * i + 8, 128 * h : 128 * h + 128]
            ritz = gram_ref[8 * i : 8 * i + 8, width + 128 * h : width + 128 * h + 128]
            ritz = ritz - 0.5 * across[8 * i : 8 * i + 8, 128 * h : 128 * h + 128]
            row = lax.broadcasted_iota(jnp.int32, (8, 128), 0) + 8 * i
            col = lax.broadcasted_iota(jnp.int32, (8, 128), 1) + 128 * h
            out_ref[17 * i + 8 * h : 17 * i + 8 * h + 8] = jnp.where(row >= col, intersection, ritz)
            if 8 * i // 128 == h:
                diagonal = jnp.sum(jnp.where(row == col, ritz, 0.0), axis=0, keepdims=True)
        out_ref[17 * i + 16 : 17 * i + 17] = diagonal


def eliminate(rows, base):
    n = len(rows)
    row = lax.broadcasted_iota(jnp.int32, (8, 128), 0)
    lane = lax.broadcasted_iota(jnp.int32, (8, 128), 1)
    pivots = []
    for p in range(n):
        c = base + 8 * p
        h, l = c // 128, c % 128
        cols = [[jnp.broadcast_to(rows[t][h][:, l + j : l + j + 1], (8, 128)) for j in range(8)] for t in range(p, n)]
        inside = (lane >= l) & (lane < l + 8)
        rows[p][h] = jnp.where(inside, jnp.where(lane - l == row, 1.0, 0.0), rows[p][h])
        for t in range(p + 1, n):
            rows[t][h] = jnp.where(inside, 0.0, rows[t][h])
        pivot = None
        for k in range(8):
            spread = lambda v: jnp.broadcast_to(v[k : k + 1, :], (8, 128))
            d = spread(cols[0][k])
            pivot = d if k == 0 else jnp.where(row >= k, d, pivot)
            r = 1.0 / d
            above = {j: spread(cols[0][j]) for j in range(k + 1, 8)}
            pivot_row = [spread(rows[p][s]) for s in range(2)]
            for t in range(p, n):
                if t == p and k == 7:
                    continue
                i = t - p
                f = cols[i][k] * r
                if t == p:
                    f = jnp.where(row > k, f, 0.0)
                for j in range(k + 1, 8):
                    cols[i][j] = cols[i][j] - f * above[j]
                for s in range(2):
                    rows[t][s] = rows[t][s] - f * pivot_row[s]
        pivots.append(pivot)
    return rows, pivots


def factor(a_ref, w_ref, g_ref):
    row = lax.broadcasted_iota(jnp.int32, (8, 128), 0)
    lane = lax.broadcasted_iota(jnp.int32, (8, 128), 1)
    width = a_ref.shape[0]
    for o in range(0, width, PANEL):
        end = o + PANEL
        rows = [[a_ref[o + 8 * t : o + 8 * t + 8, 128 * h : 128 * h + 128] for h in range(2)] for t in range(PANEL // 8)]
        rows, pivots = eliminate(rows, o)
        for t in range(PANEL // 8):
            scale = lax.rsqrt(pivots[t])
            for h in range(2):
                col = lane + 128 * h
                lower = col <= row + o + 8 * t
                g = rows[t][h] * scale
                w_ref[o + 8 * t : o + 8 * t + 8, 128 * h : 128 * h + 128] = jnp.where(lower, g, 0.0)
                g_ref[8 * t : 8 * t + 8, 128 * h : 128 * h + 128] = jnp.where(lower | (col >= end), g, 0.0)
        if end < width:
            first = end // 128 * 128
            g = g_ref[...]
            update = row_dot(g[:, first:], g, HIGHEST)[end - first :]
            col = lax.broadcasted_iota(jnp.int32, (width - end, width), 1)
            old = a_ref[end:, :]
            a_ref[end:, :] = jnp.where((col >= o) & (col < end), 0.0, old) - update


def solve_kernel(packed_ref, psi_ref, occupation_ref, count_ref, orbitals_ref, contribution_ref,
                 psi_v, out_v, a_ref, w_ref, r_ref, g_ref, in_sems, out_sems):
    rows, width = psi_ref.shape
    n = rows // CHUNK
    ins = [
        pltpu.make_async_copy(psi_ref.at[pl.ds(c * CHUNK, CHUNK)], psi_v.at[pl.ds(c * CHUNK, CHUNK)], in_sems.at[c])
        for c in range(n)
    ]
    outs = [
        pltpu.make_async_copy(out_v.at[pl.ds(c * CHUNK, CHUNK)], orbitals_ref.at[pl.ds(c * CHUNK, CHUNK)], out_sems.at[c])
        for c in range(n)
    ]
    for copy in ins:
        copy.start()
    diagonals = [jnp.zeros((1, 128), F32) for _ in range(width // 128)]
    for i in range(width // 8):
        for h in range(width // 128):
            w_ref[8 * i : 8 * i + 8, 128 * h : 128 * h + 128] = packed_ref[17 * i + 8 * h : 17 * i + 8 * h + 8]
        diagonals[8 * i // 128] += packed_ref[17 * i + 16 : 17 * i + 17]
    packed = w_ref[...]
    turned = jnp.transpose(packed)
    row = lax.broadcasted_iota(jnp.int32, (width, width), 0)
    col = lax.broadcasted_iota(jnp.int32, (width, width), 1)
    diagonal = jnp.concatenate(diagonals, axis=1)
    a_ref[...] = jnp.where(row >= col, packed, turned)
    r_ref[...] = jnp.where(row < col, packed, jnp.where(row == col, jnp.broadcast_to(diagonal, packed.shape), turned))
    factor(a_ref, w_ref, g_ref)
    inverse = w_ref[...]
    half = jnp.dot(inverse, r_ref[...], precision=HIGHEST, preferred_element_type=F32)
    projected = lax.dot_general(half, inverse, (((1,), (1,)), ((), ())), precision=HIGHEST, preferred_element_type=F32)
    identity = jnp.where(row == col, 1.0, 0.0)
    rotation = row_dot(inverse, identity - step_size * projected, HIGHEST).astype(BF16)

    state = lax.broadcasted_iota(jnp.int32, (1, width), 1)
    total = 16.0 * width
    weights = occupation_ref[...].astype(F32) * jnp.where(state < count_ref[0], 1.0, 0.0) / (2.0 * total)
    by_state = jnp.transpose(jnp.broadcast_to(weights, (128, width)))
    parts = []
    for c in range(n):
        ins[c].wait()
        for s in range(CHUNK // 256):
            start = c * CHUNK + s * 256
            psi = psi_v[start : start + 256]
            out_v[start : start + 256] = jnp.dot(psi, rotation, preferred_element_type=F32).astype(BF16)
            rotated = lax.dot_general(rotation, psi, (((0,), (1,)), ((), ())), preferred_element_type=F32)
            for h in range(2):
                piece = rotated[:, 128 * h : 128 * h + 128]
                parts.append(jnp.sum(piece * piece * by_state, axis=0, keepdims=True))
        outs[c].start()
    contribution = jnp.concatenate(parts, axis=0)
    for i in range(contribution_ref.shape[0]):
        contribution_ref[i] = contribution
    for copy in outs:
        copy.wait()


def per_device(orbitals, potential, core_density, occupation, slice_counts):
    coefficient = (3.0 / jnp.pi) ** (1.0 / 3.0)
    rows, width = orbitals.shape
    peers = lax.axis_size(GRID)
    groups = lax.axis_size("cuts")
    blocks = rows // 128
    n = rows // CHUNK
    following = lax.ppermute(orbitals[:1], GRID, [((i + 1) % peers, i) for i in range(peers)])
    potential = potential.reshape(blocks, 128)
    gram = pl.pallas_call(
        gram_kernel,
        out_shape=jax.ShapeDtypeStruct((width, 2 * width), F32),
        in_specs=[pl.BlockSpec(memory_space=pl.ANY), pl.BlockSpec(memory_space=pltpu.VMEM)],
        scratch_shapes=[
            pltpu.VMEM((rows + 2 * EDGE, width), BF16),
            pltpu.VMEM((rows, width), BF16),
            pltpu.SemaphoreType.DMA((n,)),
        ],
        name="gram",
    )(orbitals, potential)
    chunk = 17 * 128
    packed = pl.pallas_call(
        pack_kernel, out_shape=jax.ShapeDtypeStruct((17 * width // 8, 128), F32), name="pack"
    )(gram, orbitals[rows - 1 :], following)
    mine = lax.all_to_all(packed.reshape(peers, 1, chunk), GRID, 0, 0, tiled=True)
    summed = mine.sum(axis=0) / (rows * peers)
    every = lax.all_to_all(jnp.broadcast_to(summed[None], (peers, 1, chunk)), GRID, 0, 0, tiled=True)
    orbitals_out, contribution = pl.pallas_call(
        solve_kernel,
        out_shape=(
            jax.ShapeDtypeStruct((rows, width), BF16),
            jax.ShapeDtypeStruct((groups, blocks, 128), F32),
        ),
        in_specs=[
            pl.BlockSpec(memory_space=pltpu.VMEM),
            pl.BlockSpec(memory_space=pl.ANY),
            pl.BlockSpec(memory_space=pltpu.VMEM),
            pl.BlockSpec(memory_space=pltpu.SMEM),
        ],
        out_specs=(pl.BlockSpec(memory_space=pl.ANY), pl.BlockSpec(memory_space=pltpu.VMEM)),
        scratch_shapes=[
            pltpu.VMEM((rows, width), BF16),
            pltpu.VMEM((rows, width), BF16),
            pltpu.VMEM((width, width), F32),
            pltpu.VMEM((width, width), F32),
            pltpu.VMEM((width, width), F32),
            pltpu.VMEM((PANEL, width), F32),
            pltpu.SemaphoreType.DMA((n,)),
            pltpu.SemaphoreType.DMA((n,)),
        ],
        name="solve",
    )(every.reshape(17 * width // 8, 128), orbitals, occupation.reshape(1, width), slice_counts)
    density = core_density.reshape(blocks, 128) + lax.all_to_all(contribution, "cuts", 0, 0, tiled=True).sum(axis=0)
    potential_out = (1.0 - mixing) * potential + mixing * (-coefficient * jnp.cbrt(density))
    return (orbitals_out, potential_out.reshape(rows))


def solution(mesh):
    torus = Mesh(mesh.devices.reshape(mesh.shape["cuts"], 16, 2), ("cuts", "grid_0", "grid_1"))
    in_specs = (P(GRID, "cuts"), P(GRID), P(GRID), P("cuts"), P("cuts"))
    out_specs = (P(GRID, "cuts"), P(GRID))
    return jax.shard_map(
        per_device, mesh=torus, in_specs=in_specs, out_specs=out_specs, check_vma=False
    )
```

```python
import functools

import jax
import jax.numpy as jnp
from jax import lax
from jax.experimental import pallas as pl
from jax.experimental.pallas import tpu as pltpu
from jax.sharding import Mesh
from jax.sharding import PartitionSpec as P

GRID = ("grid_0", "grid_1")
HIGHEST = lax.Precision.HIGHEST
F32 = jnp.float32
BF16 = jnp.bfloat16

mixing = 0.3
step_size = 0.5

PANEL = 64
CHUNK = 1024
PIECE = 2048
EDGE = 16


def row_dot(a, b, precision=None):
    return lax.dot_general(a, b, (((0,), (0,)), ((), ())), precision=precision, preferred_element_type=F32)


def gram_kernel(psi_ref, potential_ref, out_ref, last_ref, psi_v, applied_v, sems):
    rows, width = psi_ref.shape
    n = rows // CHUNK
    copies = [
        pltpu.make_async_copy(
            psi_ref.at[pl.ds(c * CHUNK, CHUNK)], psi_v.at[pl.ds(EDGE + c * CHUNK, CHUNK)], sems.at[c]
        )
        for c in range(n)
    ]
    for copy in copies:
        copy.start()
    psi_v[0:EDGE] = jnp.zeros((EDGE, width), BF16)
    psi_v[EDGE + rows : EDGE + rows + EDGE] = jnp.zeros((EDGE, width), BF16)
    by_row = jnp.transpose(potential_ref[...])
    intersection = ritz = None
    copies[0].wait()
    for c in range(n + 1):
        if c + 1 < n:
            copies[c + 1].wait()
        if c < n:
            for s in range(CHUNK // 128):
                start = c * CHUNK + s * 128
                block = start // 128
                wide = psi_v[start : start + 128 + 2 * EDGE].astype(F32)
                length = wide.shape[0]
                after = pltpu.roll(wide, length - 1, 0)[EDGE : EDGE + 128]
                before = pltpu.roll(wide, 1, 0)[EDGE : EDGE + 128]
                middle = wide[EDGE : EDGE + 128]
                kinetic = -0.5 * (after + before - 2.0 * middle)
                applied_v[start : start + 128] = (kinetic + by_row[:, block : block + 1] * middle).astype(BF16)
            psi = psi_v[EDGE + c * CHUNK : EDGE + (c + 1) * CHUNK]
            one = row_dot(psi, psi)
            intersection = one if c == 0 else intersection + one
        if c > 0:
            psi = psi_v[EDGE + (c - 1) * CHUNK : EDGE + c * CHUNK]
            one = row_dot(psi, applied_v[(c - 1) * CHUNK : c * CHUNK])
            ritz = one if c == 1 else ritz + one
    row = lax.broadcasted_iota(jnp.int32, (8, 128), 0)
    col = lax.broadcasted_iota(jnp.int32, (8, 128), 1)
    for i in range(width // 8):
        for h in range(width // 128):
            one = intersection[8 * i : 8 * i + 8, 128 * h : 128 * h + 128]
            two = ritz[8 * i : 8 * i + 8, 128 * h : 128 * h + 128]
            out_ref[17 * i + 8 * h : 17 * i + 8 * h + 8] = jnp.where(row + 8 * i >= col + 128 * h, one, two)
            if 8 * i // 128 == h:
                diagonal = jnp.sum(jnp.where(row + 8 * i == col + 128 * h, two, 0.0), axis=0, keepdims=True)
        out_ref[17 * i + 16 : 17 * i + 17] = diagonal
    last_ref[...] = psi_v[rows : rows + EDGE]


def border_kernel(packed_ref, last_ref, next_ref, out_ref):
    width = last_ref.shape[1]
    zeros = jnp.zeros((14, width), F32)
    last, following = last_ref[...].astype(F32)[EDGE - 1 :], next_ref[...].astype(F32)[:1]
    left = jnp.concatenate([last, following, zeros], axis=0).astype(BF16)
    right = jnp.concatenate([following, last, zeros], axis=0).astype(BF16)
    across = -0.5 * row_dot(left, right)
    row = lax.broadcasted_iota(jnp.int32, (8, 128), 0)
    col = lax.broadcasted_iota(jnp.int32, (8, 128), 1)
    for i in range(width // 8):
        for h in range(width // 128):
            place = slice(17 * i + 8 * h, 17 * i + 8 * h + 8)
            piece = across[8 * i : 8 * i + 8, 128 * h : 128 * h + 128]
            if 8 * i >= 128 * (h + 1):
                out_ref[place] = packed_ref[place]
            else:
                out_ref[place] = packed_ref[place] + jnp.where(row + 8 * i < col + 128 * h, piece, 0.0)
            if 8 * i // 128 == h:
                diagonal = jnp.sum(jnp.where(row + 8 * i == col + 128 * h, piece, 0.0), axis=0, keepdims=True)
        place = slice(17 * i + 16, 17 * i + 17)
        out_ref[place] = packed_ref[place] + diagonal


def spread_kernel(points, arrived_ref, out_ref):
    peers = arrived_ref.shape[0]
    total = arrived_ref[0]
    for i in range(1, peers):
        total = total + arrived_ref[i]
    total = total * (1.0 / points)
    for i in range(peers):
        out_ref[i] = total


def eliminate(rows, base):
    n = len(rows)
    row = lax.broadcasted_iota(jnp.int32, (8, 128), 0)
    lane = lax.broadcasted_iota(jnp.int32, (8, 128), 1)
    pivots = []

    def columns(t, c, count):
        h, l = c // 128, c % 128
        return [jnp.broadcast_to(rows[t][h][:, l + j : l + j + 1], (8, 128)) for j in range(count)]

    def replaced(t, c, diagonal):
        h, l = c // 128, c % 128
        inside = (lane >= l) & (lane < l + 8)
        rows[t][h] = jnp.where(inside, jnp.where(lane - l == row, 1.0, 0.0) if diagonal else 0.0, rows[t][h])

    for p in range(0, n, 2):
        c = base + 8 * p
        cols = [columns(p + q, c, 16) for q in range(2)]
        replaced(p, c, True)
        replaced(p + 1, c, False)
        steps = []
        for k in range(16):
            q, m = k // 8, k % 8
            spread = lambda v: jnp.broadcast_to(v[m : m + 1, :], (8, 128))
            if k == 8:
                replaced(p + 1, c + 8, True)
            d = spread(cols[q][k])
            pivot = d if m == 0 else jnp.where(row >= m, d, pivot)
            r = 1.0 / d
            above = {j: spread(cols[q][j]) for j in range(k + 1, 16)}
            pivot_row = [spread(rows[p + q][s]) for s in range(2)]
            steps.append((r, above, pivot_row))
            for i in range(q, 2):
                if i == q and m == 7:
                    continue
                f = cols[i][k] * r
                if i == q:
                    f = jnp.where(row > m, f, 0.0)
                for j in range(k + 1, 16):
                    cols[i][j] = cols[i][j] - f * above[j]
                for s in range(2):
                    rows[p + i][s] = rows[p + i][s] - f * pivot_row[s]
            if m == 7:
                pivots.append(pivot)
        for t in range(p + 2, n):
            for q in range(2):
                mine = columns(t, c + 8 * q, 8)
                replaced(t, c + 8 * q, False)
                for m in range(8):
                    r, above, pivot_row = steps[8 * q + m]
                    f = mine[m] * r
                    for j in range(m + 1, 8):
                        mine[j] = mine[j] - f * above[8 * q + j]
                    for s in range(2):
                        rows[t][s] = rows[t][s] - f * pivot_row[s]
    return rows, pivots


def factor(a_ref, w_ref, g_ref):
    row = lax.broadcasted_iota(jnp.int32, (8, 128), 0)
    lane = lax.broadcasted_iota(jnp.int32, (8, 128), 1)
    width = a_ref.shape[0]
    for o in range(0, width, PANEL):
        end = o + PANEL
        rows = [[a_ref[o + 8 * t : o + 8 * t + 8, 128 * h : 128 * h + 128] for h in range(2)] for t in range(PANEL // 8)]
        rows, pivots = eliminate(rows, o)
        for t in range(PANEL // 8):
            scale = lax.rsqrt(pivots[t])
            for h in range(2):
                col = lane + 128 * h
                lower = col <= row + o + 8 * t
                g = rows[t][h] * scale
                w_ref[o + 8 * t : o + 8 * t + 8, 128 * h : 128 * h + 128] = jnp.where(lower, g, 0.0)
                g_ref[8 * t : 8 * t + 8, 128 * h : 128 * h + 128] = jnp.where(lower | (col >= end), g, 0.0)
        if end < width:
            first = end // 128 * 128
            g = g_ref[...]
            update = row_dot(g[:, first:], g, HIGHEST)[end - first :]
            col = lax.broadcasted_iota(jnp.int32, (width - end, width), 1)
            old = a_ref[end:, :]
            a_ref[end:, :] = jnp.where((col >= o) & (col < end), 0.0, old) - update


def solve_kernel(packed_ref, psi_ref, occupation_ref, count_ref, orbitals_ref, contribution_ref,
                 psi_v, out_v, a_ref, w_ref, r_ref, g_ref, in_sems, out_sems):
    rows, width = psi_ref.shape
    n = rows // PIECE
    ins = [
        pltpu.make_async_copy(psi_ref.at[pl.ds(c * PIECE, PIECE)], psi_v.at[pl.ds(c * PIECE, PIECE)], in_sems.at[c])
        for c in range(n)
    ]
    outs = [
        pltpu.make_async_copy(out_v.at[pl.ds(c * PIECE, PIECE)], orbitals_ref.at[pl.ds(c * PIECE, PIECE)], out_sems.at[c])
        for c in range(n)
    ]
    for copy in ins:
        copy.start()
    diagonals = [jnp.zeros((1, 128), F32) for _ in range(width // 128)]
    for i in range(width // 8):
        for h in range(width // 128):
            w_ref[8 * i : 8 * i + 8, 128 * h : 128 * h + 128] = packed_ref[17 * i + 8 * h : 17 * i + 8 * h + 8]
        diagonals[8 * i // 128] += packed_ref[17 * i + 16 : 17 * i + 17]
    packed = w_ref[...]
    turned = jnp.transpose(packed)
    row = lax.broadcasted_iota(jnp.int32, (width, width), 0)
    col = lax.broadcasted_iota(jnp.int32, (width, width), 1)
    diagonal = jnp.concatenate(diagonals, axis=1)
    a_ref[...] = jnp.where(row >= col, packed, turned)
    r_ref[...] = jnp.where(row < col, packed, jnp.where(row == col, jnp.broadcast_to(diagonal, packed.shape), turned))
    factor(a_ref, w_ref, g_ref)
    inverse = w_ref[...]
    half = jnp.dot(inverse, r_ref[...], precision=HIGHEST, preferred_element_type=F32)
    projected = lax.dot_general(half, inverse, (((1,), (1,)), ((), ())), precision=HIGHEST, preferred_element_type=F32)
    identity = jnp.where(row == col, 1.0, 0.0)
    rotation = row_dot(inverse, identity - step_size * projected, HIGHEST).astype(BF16)

    state = lax.broadcasted_iota(jnp.int32, (1, width), 1)
    total = 16.0 * width
    weights = occupation_ref[...].astype(F32) * jnp.where(state < count_ref[...], 1.0, 0.0) / (2.0 * total)
    on_diagonal = lax.broadcasted_iota(jnp.int32, (128, 128), 0) == lax.broadcasted_iota(jnp.int32, (128, 128), 1)
    parts = []
    for c in range(n):
        ins[c].wait()
        for s in range(PIECE // 256):
            start = c * PIECE + s * 256
            rotated = jnp.dot(psi_v[start : start + 256], rotation, preferred_element_type=F32)
            out_v[start : start + 256] = rotated.astype(BF16)
            weighted = rotated * rotated * weights
            weighted = weighted[:, :128] + weighted[:, 128:]
            for h in range(2):
                sums = jnp.sum(weighted[128 * h : 128 * h + 128], axis=1, keepdims=True)
                parts.append(jnp.sum(jnp.where(on_diagonal, sums, 0.0), axis=0, keepdims=True))
        outs[c].start()
    contribution = jnp.concatenate(parts, axis=0)
    for i in range(contribution_ref.shape[0]):
        contribution_ref[i] = contribution
    for copy in outs:
        copy.wait()


def in_vmem(x):
    return pltpu.with_memory_space_constraint(x, pltpu.VMEM)


def per_device(orbitals, potential, core_density, occupation, slice_counts):
    coefficient = (3.0 / jnp.pi) ** (1.0 / 3.0)
    rows, width = orbitals.shape
    peers = lax.axis_size(GRID)
    groups = lax.axis_size("cuts")
    blocks = rows // 128
    n = rows // CHUNK
    following = lax.ppermute(orbitals[:8], GRID, [((i + 1) % peers, i) for i in range(peers)])
    potential = potential.reshape(blocks, 128)
    packed, last = pl.pallas_call(
        gram_kernel,
        out_shape=(pltpu.VMEM((17 * width // 8, 128), F32), pltpu.VMEM((EDGE, width), BF16)),
        in_specs=[pl.BlockSpec(memory_space=pl.ANY), pl.BlockSpec(memory_space=pltpu.VMEM)],
        scratch_shapes=[
            pltpu.VMEM((rows + 2 * EDGE, width), BF16),
            pltpu.VMEM((rows, width), BF16),
            pltpu.SemaphoreType.DMA((n,)),
        ],
        name="gram",
    )(orbitals, potential)
    chunk = 17 * 128
    packed = pl.pallas_call(border_kernel, out_shape=pltpu.VMEM((17 * width // 8, 128), F32), name="border")(
        in_vmem(packed), in_vmem(last), in_vmem(following)
    )
    mine = lax.all_to_all(packed.reshape(peers, 1, chunk), GRID, 0, 0, tiled=True)
    copies = pl.pallas_call(functools.partial(spread_kernel, rows * peers), out_shape=pltpu.VMEM((peers, 1, chunk), F32), name="spread")(in_vmem(mine))
    every = lax.all_to_all(copies, GRID, 0, 0, tiled=True)
    orbitals_out, contribution = pl.pallas_call(
        solve_kernel,
        out_shape=(
            jax.ShapeDtypeStruct((rows, width), BF16),
            pltpu.VMEM((groups, blocks, 128), F32),
        ),
        in_specs=[
            pl.BlockSpec(memory_space=pltpu.VMEM),
            pl.BlockSpec(memory_space=pl.ANY),
            pl.BlockSpec(memory_space=pltpu.VMEM),
            pl.BlockSpec(memory_space=pltpu.VMEM),
        ],
        out_specs=(pl.BlockSpec(memory_space=pl.ANY), pl.BlockSpec(memory_space=pltpu.VMEM)),
        scratch_shapes=[
            pltpu.VMEM((rows, width), BF16),
            pltpu.VMEM((rows, width), BF16),
            pltpu.VMEM((width, width), F32),
            pltpu.VMEM((width, width), F32),
            pltpu.VMEM((width, width), F32),
            pltpu.VMEM((PANEL, width), F32),
            pltpu.SemaphoreType.DMA((rows // PIECE,)),
            pltpu.SemaphoreType.DMA((rows // PIECE,)),
        ],
        name="solve",
    )(in_vmem(every.reshape(17 * width // 8, 128)), orbitals, occupation.reshape(1, width), slice_counts.reshape(1, 1))
    density = core_density.reshape(blocks, 128) + lax.all_to_all(contribution, "cuts", 0, 0, tiled=True).sum(axis=0)
    potential_out = (1.0 - mixing) * potential + mixing * (-coefficient * jnp.cbrt(density))
    return (orbitals_out, potential_out.reshape(rows))


def solution(mesh):
    torus = Mesh(mesh.devices.reshape(mesh.shape["cuts"], 16, 2), ("cuts", "grid_0", "grid_1"))
    in_specs = (P(GRID, "cuts"), P(GRID), P(GRID), P("cuts"), P("cuts"))
    out_specs = (P(GRID, "cuts"), P(GRID))
    return jax.shard_map(
        per_device, mesh=torus, in_specs=in_specs, out_specs=out_specs, check_vma=False
    )
```

```python
import functools

import jax
import jax.numpy as jnp
from jax import lax
from jax.experimental import pallas as pl
from jax.experimental.pallas import tpu as pltpu
from jax.sharding import Mesh
from jax.sharding import PartitionSpec as P

GRID = ("grid_0", "grid_1")
HIGHEST = lax.Precision.HIGHEST
F32 = jnp.float32
BF16 = jnp.bfloat16

mixing = 0.3
step_size = 0.5

PANEL = 64
CHUNK = 1024
PIECE = 2048
EDGE = 16


def row_dot(a, b, precision=None):
    return lax.dot_general(a, b, (((0,), (0,)), ((), ())), precision=precision, preferred_element_type=F32)


def gram_kernel(total_states, psi_ref, potential_ref, occupation_ref, count_ref, out_ref, last_ref, weights_ref, applied_v):
    rows, width = psi_ref.shape
    n = rows // CHUNK
    state = lax.broadcasted_iota(jnp.int32, (1, width), 1)
    live = jnp.where(state < count_ref[...], 1.0, 0.0)
    weights_ref[...] = occupation_ref[...].astype(F32) * live / (2.0 * total_states)
    by_row = jnp.transpose(potential_ref[...])
    outside = jnp.zeros((EDGE, width), BF16)
    intersection = ritz = None
    for c in range(n + 1):
        if c < n:
            for s in range(CHUNK // 128):
                start = c * CHUNK + s * 128
                block = start // 128
                if start == 0:
                    wide = jnp.concatenate([outside, psi_ref[0 : 128 + EDGE]], axis=0).astype(F32)
                elif start + 128 == rows:
                    wide = jnp.concatenate([psi_ref[start - EDGE : rows], outside], axis=0).astype(F32)
                else:
                    wide = psi_ref[start - EDGE : start + 128 + EDGE].astype(F32)
                length = wide.shape[0]
                after = pltpu.roll(wide, length - 1, 0)[EDGE : EDGE + 128]
                before = pltpu.roll(wide, 1, 0)[EDGE : EDGE + 128]
                middle = wide[EDGE : EDGE + 128]
                kinetic = -0.5 * (after + before - 2.0 * middle)
                applied_v[start : start + 128] = (kinetic + by_row[:, block : block + 1] * middle).astype(BF16)
            psi = psi_ref[c * CHUNK : (c + 1) * CHUNK]
            one = row_dot(psi, psi)
            intersection = one if c == 0 else intersection + one
        if c > 0:
            psi = psi_ref[(c - 1) * CHUNK : c * CHUNK]
            one = row_dot(psi, applied_v[(c - 1) * CHUNK : c * CHUNK])
            ritz = one if c == 1 else ritz + one
    row = lax.broadcasted_iota(jnp.int32, (8, 128), 0)
    col = lax.broadcasted_iota(jnp.int32, (8, 128), 1)
    for i in range(width // 8):
        for h in range(width // 128):
            one = intersection[8 * i : 8 * i + 8, 128 * h : 128 * h + 128]
            two = ritz[8 * i : 8 * i + 8, 128 * h : 128 * h + 128]
            out_ref[17 * i + 8 * h : 17 * i + 8 * h + 8] = jnp.where(row + 8 * i >= col + 128 * h, one, two)
            if 8 * i // 128 == h:
                diagonal = jnp.sum(jnp.where(row + 8 * i == col + 128 * h, two, 0.0), axis=0, keepdims=True)
        out_ref[17 * i + 16 : 17 * i + 17] = diagonal
    last_ref[...] = psi_ref[rows - EDGE : rows]


def border_kernel(packed_ref, last_ref, next_ref, out_ref):
    width = last_ref.shape[1]
    zeros = jnp.zeros((14, width), F32)
    last, following = last_ref[...].astype(F32)[EDGE - 1 :], next_ref[...].astype(F32)[:1]
    left = jnp.concatenate([last, following, zeros], axis=0).astype(BF16)
    right = jnp.concatenate([following, last, zeros], axis=0).astype(BF16)
    across = -0.5 * row_dot(left, right)
    row = lax.broadcasted_iota(jnp.int32, (8, 128), 0)
    col = lax.broadcasted_iota(jnp.int32, (8, 128), 1)
    for i in range(width // 8):
        for h in range(width // 128):
            place = slice(17 * i + 8 * h, 17 * i + 8 * h + 8)
            piece = across[8 * i : 8 * i + 8, 128 * h : 128 * h + 128]
            if 8 * i >= 128 * (h + 1):
                out_ref[place] = packed_ref[place]
            else:
                out_ref[place] = packed_ref[place] + jnp.where(row + 8 * i < col + 128 * h, piece, 0.0)
            if 8 * i // 128 == h:
                diagonal = jnp.sum(jnp.where(row + 8 * i == col + 128 * h, piece, 0.0), axis=0, keepdims=True)
        place = slice(17 * i + 16, 17 * i + 17)
        out_ref[place] = packed_ref[place] + diagonal


def spread_kernel(points, arrived_ref, out_ref):
    peers = arrived_ref.shape[0]
    total = arrived_ref[0]
    for i in range(1, peers):
        total = total + arrived_ref[i]
    total = total * (1.0 / points)
    for i in range(peers):
        out_ref[i] = total


def eliminate(rows, base):
    n = len(rows)
    row = lax.broadcasted_iota(jnp.int32, (8, 128), 0)
    lane = lax.broadcasted_iota(jnp.int32, (8, 128), 1)
    pivots = []

    def columns(t, c, count):
        h, l = c // 128, c % 128
        return [jnp.broadcast_to(rows[t][h][:, l + j : l + j + 1], (8, 128)) for j in range(count)]

    def replaced(t, c, diagonal):
        h, l = c // 128, c % 128
        inside = (lane >= l) & (lane < l + 8)
        rows[t][h] = jnp.where(inside, jnp.where(lane - l == row, 1.0, 0.0) if diagonal else 0.0, rows[t][h])

    for p in range(0, n, 2):
        c = base + 8 * p
        cols = [columns(p + q, c, 16) for q in range(2)]
        replaced(p, c, True)
        replaced(p + 1, c, False)
        steps = []
        for k in range(16):
            q, m = k // 8, k % 8
            spread = lambda v: jnp.broadcast_to(v[m : m + 1, :], (8, 128))
            if k == 8:
                replaced(p + 1, c + 8, True)
            d = spread(cols[q][k])
            pivot = d if m == 0 else jnp.where(row >= m, d, pivot)
            r = 1.0 / d
            above = {j: spread(cols[q][j]) for j in range(k + 1, 16)}
            pivot_row = [spread(rows[p + q][s]) for s in range(2)]
            steps.append((r, above, pivot_row))
            for i in range(q, 2):
                if i == q and m == 7:
                    continue
                f = cols[i][k] * r
                for j in range(k + 1, 16):
                    if j == k + 1:
                        cols[i][j] = cols[i][j] - cols[i][k] * above[j] * r
                    else:
                        cols[i][j] = cols[i][j] - f * above[j]
                if i == q:
                    f = jnp.where(row > m, f, 0.0)
                for s in range(2):
                    rows[p + i][s] = rows[p + i][s] - f * pivot_row[s]
            if m == 7:
                pivots.append(pivot)
        for t in range(p + 2, n):
            for q in range(2):
                mine = columns(t, c + 8 * q, 8)
                replaced(t, c + 8 * q, False)
                for m in range(8):
                    r, above, pivot_row = steps[8 * q + m]
                    f = mine[m] * r
                    for j in range(m + 1, 8):
                        mine[j] = mine[j] - f * above[8 * q + j]
                    for s in range(2):
                        rows[t][s] = rows[t][s] - f * pivot_row[s]
    return rows, pivots


def factor(a_ref, w_ref, g_ref):
    row = lax.broadcasted_iota(jnp.int32, (8, 128), 0)
    lane = lax.broadcasted_iota(jnp.int32, (8, 128), 1)
    width = a_ref.shape[0]
    for o in range(0, width, PANEL):
        end = o + PANEL
        rows = [[a_ref[o + 8 * t : o + 8 * t + 8, 128 * h : 128 * h + 128] for h in range(2)] for t in range(PANEL // 8)]
        rows, pivots = eliminate(rows, o)
        for t in range(PANEL // 8):
            scale = lax.rsqrt(pivots[t])
            for h in range(2):
                col = lane + 128 * h
                lower = col <= row + o + 8 * t
                g = rows[t][h] * scale
                w_ref[o + 8 * t : o + 8 * t + 8, 128 * h : 128 * h + 128] = jnp.where(lower, g, 0.0)
                g_ref[8 * t : 8 * t + 8, 128 * h : 128 * h + 128] = jnp.where(lower | (col >= end), g, 0.0)
        if end < width:
            g = g_ref[...]
            bounds = (end, end + PANEL, width) if end + PANEL < width else (end, width)
            for low, high in zip(bounds, bounds[1:]):
                first, last = low // 128 * 128, -(-high // 128) * 128
                update = row_dot(g[:, first:last], g, HIGHEST)[low - first : high - first]
                col = lax.broadcasted_iota(jnp.int32, (high - low, width), 1)
                a_ref[low:high, :] = jnp.where((col >= o) & (col < end), 0.0, a_ref[low:high, :]) - update


def solve_kernel(packed_ref, psi_ref, weights_ref, orbitals_ref, contribution_ref,
                 psi_v, out_v, a_ref, w_ref, r_ref, g_ref, in_sems, out_sems):
    rows, width = psi_ref.shape
    n = rows // PIECE
    ins = [
        pltpu.make_async_copy(psi_ref.at[pl.ds(c * PIECE, PIECE)], psi_v.at[pl.ds(c * PIECE, PIECE)], in_sems.at[c])
        for c in range(n)
    ]
    outs = [
        pltpu.make_async_copy(out_v.at[pl.ds(c * PIECE, PIECE)], orbitals_ref.at[pl.ds(c * PIECE, PIECE)], out_sems.at[c])
        for c in range(n)
    ]
    for copy in ins:
        copy.start()
    diagonals = [jnp.zeros((1, 128), F32) for _ in range(width // 128)]
    for i in range(width // 8):
        for h in range(width // 128):
            w_ref[8 * i : 8 * i + 8, 128 * h : 128 * h + 128] = packed_ref[17 * i + 8 * h : 17 * i + 8 * h + 8]
        diagonals[8 * i // 128] += packed_ref[17 * i + 16 : 17 * i + 17]
    packed = w_ref[...]
    turned = jnp.transpose(packed)
    row = lax.broadcasted_iota(jnp.int32, (width, width), 0)
    col = lax.broadcasted_iota(jnp.int32, (width, width), 1)
    diagonal = jnp.concatenate(diagonals, axis=1)
    a_ref[...] = jnp.where(row >= col, packed, turned)
    r_ref[...] = jnp.where(row < col, packed, jnp.where(row == col, jnp.broadcast_to(diagonal, packed.shape), turned))
    factor(a_ref, w_ref, g_ref)
    inverse = w_ref[...]
    half = jnp.dot(inverse, r_ref[...], precision=HIGHEST, preferred_element_type=F32)
    projected = lax.dot_general(half, inverse, (((1,), (1,)), ((), ())), precision=HIGHEST, preferred_element_type=F32)
    identity = jnp.where(row == col, 1.0, 0.0)
    rotation = row_dot(inverse, identity - step_size * projected, HIGHEST).astype(BF16)

    weights = weights_ref[...]
    on_diagonal = lax.broadcasted_iota(jnp.int32, (128, 128), 0) == lax.broadcasted_iota(jnp.int32, (128, 128), 1)
    parts = []
    for c in range(n):
        ins[c].wait()
        for s in range(PIECE // 256):
            start = c * PIECE + s * 256
            rotated = jnp.dot(psi_v[start : start + 256], rotation, preferred_element_type=F32)
            out_v[start : start + 256] = rotated.astype(BF16)
            weighted = rotated * rotated * weights
            weighted = weighted[:, :128] + weighted[:, 128:]
            for h in range(2):
                sums = jnp.sum(weighted[128 * h : 128 * h + 128], axis=1, keepdims=True)
                parts.append(jnp.sum(jnp.where(on_diagonal, sums, 0.0), axis=0, keepdims=True))
        outs[c].start()
    contribution = jnp.concatenate(parts, axis=0)
    for i in range(contribution_ref.shape[0]):
        contribution_ref[i] = contribution
    for copy in outs:
        copy.wait()


def in_vmem(x):
    return pltpu.with_memory_space_constraint(x, pltpu.VMEM)


def per_device(orbitals, potential, core_density, occupation, slice_counts):
    coefficient = (3.0 / jnp.pi) ** (1.0 / 3.0)
    rows, width = orbitals.shape
    peers = lax.axis_size(GRID)
    groups = lax.axis_size("cuts")
    blocks = rows // 128
    following = lax.ppermute(orbitals[:8], GRID, [((i + 1) % peers, i) for i in range(peers)])
    potential = potential.reshape(blocks, 128)
    packed, last, weights = pl.pallas_call(
        functools.partial(gram_kernel, width * groups),
        out_shape=(
            pltpu.VMEM((17 * width // 8, 128), F32),
            pltpu.VMEM((EDGE, width), BF16),
            pltpu.VMEM((1, width), F32),
        ),
        scratch_shapes=[pltpu.VMEM((rows, width), BF16)],
        name="gram",
    )(in_vmem(orbitals), potential, occupation.reshape(1, width), slice_counts.reshape(1, 1))
    chunk = 17 * 128
    packed = pl.pallas_call(border_kernel, out_shape=pltpu.VMEM((17 * width // 8, 128), F32), name="border")(
        in_vmem(packed), in_vmem(last), in_vmem(following)
    )
    mine = lax.all_to_all(packed.reshape(peers, 1, chunk), GRID, 0, 0, tiled=True)
    copies = pl.pallas_call(functools.partial(spread_kernel, rows * peers), out_shape=pltpu.VMEM((peers, 1, chunk), F32), name="spread")(in_vmem(mine))
    every = lax.all_to_all(copies, GRID, 0, 0, tiled=True)
    orbitals_out, contribution = pl.pallas_call(
        solve_kernel,
        out_shape=(
            jax.ShapeDtypeStruct((rows, width), BF16),
            pltpu.VMEM((groups, blocks, 128), F32),
        ),
        in_specs=[
            pl.BlockSpec(memory_space=pltpu.VMEM),
            pl.BlockSpec(memory_space=pl.ANY),
            pl.BlockSpec(memory_space=pltpu.VMEM),
        ],
        out_specs=(pl.BlockSpec(memory_space=pl.ANY), pl.BlockSpec(memory_space=pltpu.VMEM)),
        scratch_shapes=[
            pltpu.VMEM((rows, width), BF16),
            pltpu.VMEM((rows, width), BF16),
            pltpu.VMEM((width, width), F32),
            pltpu.VMEM((width, width), F32),
            pltpu.VMEM((width, width), F32),
            pltpu.VMEM((PANEL, width), F32),
            pltpu.SemaphoreType.DMA((rows // PIECE,)),
            pltpu.SemaphoreType.DMA((rows // PIECE,)),
        ],
        name="solve",
    )(in_vmem(every.reshape(17 * width // 8, 128)), orbitals, in_vmem(weights))
    density = core_density.reshape(blocks, 128) + lax.all_to_all(contribution, "cuts", 0, 0, tiled=True).sum(axis=0)
    potential_out = (1.0 - mixing) * potential + mixing * (-coefficient * jnp.cbrt(density))
    return (orbitals_out, potential_out.reshape(rows))


def solution(mesh):
    torus = Mesh(mesh.devices.reshape(mesh.shape["cuts"], 16, 2), ("cuts", "grid_0", "grid_1"))
    in_specs = (P(GRID, "cuts"), P(GRID), P(GRID), P("cuts"), P("cuts"))
    out_specs = (P(GRID, "cuts"), P(GRID))
    return jax.shard_map(
        per_device, mesh=torus, in_specs=in_specs, out_specs=out_specs, check_vma=False
    )
```

```python
import functools

import jax
import jax.numpy as jnp
from jax import lax
from jax.experimental import pallas as pl
from jax.experimental.pallas import tpu as pltpu
from jax.sharding import Mesh
from jax.sharding import PartitionSpec as P

GRID = ("z_hi", "z_lo", "x_lo")
EXCHANGE = ('z_lo', 'z_hi', 'x_lo')
HIGHEST = lax.Precision.HIGHEST
F32 = jnp.float32
BF16 = jnp.bfloat16

mixing = 0.3
step_size = 0.5

PANEL = 64
CHUNK = 1024
PIECE = 2048
EDGE = 16


def row_dot(a, b, precision=None):
    return lax.dot_general(a, b, (((0,), (0,)), ((), ())), precision=precision, preferred_element_type=F32)


def gram_kernel(total_states, psi_ref, potential_ref, occupation_ref, count_ref, out_ref, last_ref, weights_ref, applied_v):
    rows, width = psi_ref.shape
    n = rows // CHUNK
    state = lax.broadcasted_iota(jnp.int32, (1, width), 1)
    live = jnp.where(state < count_ref[...], 1.0, 0.0)
    weights_ref[...] = occupation_ref[...].astype(F32) * live / (2.0 * total_states)
    by_row = jnp.transpose(potential_ref[...])
    outside = jnp.zeros((EDGE, width), BF16)
    intersection = ritz = None
    for c in range(n + 1):
        if c < n:
            for s in range(CHUNK // 128):
                start = c * CHUNK + s * 128
                block = start // 128
                if start == 0:
                    wide = jnp.concatenate([outside, psi_ref[0 : 128 + EDGE]], axis=0).astype(F32)
                elif start + 128 == rows:
                    wide = jnp.concatenate([psi_ref[start - EDGE : rows], outside], axis=0).astype(F32)
                else:
                    wide = psi_ref[start - EDGE : start + 128 + EDGE].astype(F32)
                length = wide.shape[0]
                after = pltpu.roll(wide, length - 1, 0)[EDGE : EDGE + 128]
                before = pltpu.roll(wide, 1, 0)[EDGE : EDGE + 128]
                middle = wide[EDGE : EDGE + 128]
                kinetic = -0.5 * (after + before - 2.0 * middle)
                applied_v[start : start + 128] = (kinetic + by_row[:, block : block + 1] * middle).astype(BF16)
            psi = psi_ref[c * CHUNK : (c + 1) * CHUNK]
            one = row_dot(psi, psi)
            intersection = one if c == 0 else intersection + one
        if c > 0:
            psi = psi_ref[(c - 1) * CHUNK : c * CHUNK]
            one = row_dot(psi, applied_v[(c - 1) * CHUNK : c * CHUNK])
            ritz = one if c == 1 else ritz + one
    row = lax.broadcasted_iota(jnp.int32, (8, 128), 0)
    col = lax.broadcasted_iota(jnp.int32, (8, 128), 1)
    for i in range(width // 8):
        for h in range(width // 128):
            one = intersection[8 * i : 8 * i + 8, 128 * h : 128 * h + 128]
            two = ritz[8 * i : 8 * i + 8, 128 * h : 128 * h + 128]
            out_ref[17 * i + 8 * h : 17 * i + 8 * h + 8] = jnp.where(row + 8 * i >= col + 128 * h, one, two)
            if 8 * i // 128 == h:
                diagonal = jnp.sum(jnp.where(row + 8 * i == col + 128 * h, two, 0.0), axis=0, keepdims=True)
        out_ref[17 * i + 16 : 17 * i + 17] = diagonal
    last_ref[...] = psi_ref[rows - EDGE : rows]


def border_kernel(packed_ref, last_ref, next_ref, out_ref):
    width = last_ref.shape[1]
    zeros = jnp.zeros((14, width), F32)
    last, following = last_ref[...].astype(F32)[EDGE - 1 :], next_ref[...].astype(F32)[:1]
    left = jnp.concatenate([last, following, zeros], axis=0).astype(BF16)
    right = jnp.concatenate([following, last, zeros], axis=0).astype(BF16)
    across = -0.5 * row_dot(left, right)
    row = lax.broadcasted_iota(jnp.int32, (8, 128), 0)
    col = lax.broadcasted_iota(jnp.int32, (8, 128), 1)
    for i in range(width // 8):
        for h in range(width // 128):
            place = slice(17 * i + 8 * h, 17 * i + 8 * h + 8)
            piece = across[8 * i : 8 * i + 8, 128 * h : 128 * h + 128]
            if 8 * i >= 128 * (h + 1):
                out_ref[place] = packed_ref[place]
            else:
                out_ref[place] = packed_ref[place] + jnp.where(row + 8 * i < col + 128 * h, piece, 0.0)
            if 8 * i // 128 == h:
                diagonal = jnp.sum(jnp.where(row + 8 * i == col + 128 * h, piece, 0.0), axis=0, keepdims=True)
        place = slice(17 * i + 16, 17 * i + 17)
        out_ref[place] = packed_ref[place] + diagonal


def spread_kernel(points, arrived_ref, out_ref):
    peers = arrived_ref.shape[0]
    total = arrived_ref[0]
    for i in range(1, peers):
        total = total + arrived_ref[i]
    total = total * (1.0 / points)
    for i in range(peers):
        out_ref[i] = total


def eliminate(rows, base):
    n = len(rows)
    row = lax.broadcasted_iota(jnp.int32, (8, 128), 0)
    lane = lax.broadcasted_iota(jnp.int32, (8, 128), 1)
    pivots = []

    def columns(t, c, count):
        h, l = c // 128, c % 128
        return [jnp.broadcast_to(rows[t][h][:, l + j : l + j + 1], (8, 128)) for j in range(count)]

    def replaced(t, c, diagonal):
        h, l = c // 128, c % 128
        inside = (lane >= l) & (lane < l + 8)
        rows[t][h] = jnp.where(inside, jnp.where(lane - l == row, 1.0, 0.0) if diagonal else 0.0, rows[t][h])

    for p in range(0, n, 2):
        c = base + 8 * p
        cols = [columns(p + q, c, 16) for q in range(2)]
        replaced(p, c, True)
        replaced(p + 1, c, False)
        steps = []
        for k in range(16):
            q, m = k // 8, k % 8
            spread = lambda v: jnp.broadcast_to(v[m : m + 1, :], (8, 128))
            if k == 8:
                replaced(p + 1, c + 8, True)
            d = spread(cols[q][k])
            pivot = d if m == 0 else jnp.where(row >= m, d, pivot)
            r = 1.0 / d
            above = {j: spread(cols[q][j]) for j in range(k + 1, 16)}
            pivot_row = [spread(rows[p + q][s]) for s in range(2)]
            steps.append((r, above, pivot_row))
            for i in range(q, 2):
                if i == q and m == 7:
                    continue
                f = cols[i][k] * r
                for j in range(k + 1, 16):
                    if j == k + 1:
                        cols[i][j] = cols[i][j] - cols[i][k] * above[j] * r
                    else:
                        cols[i][j] = cols[i][j] - f * above[j]
                if i == q:
                    f = jnp.where(row > m, f, 0.0)
                for s in range(2):
                    rows[p + i][s] = rows[p + i][s] - f * pivot_row[s]
            if m == 7:
                pivots.append(pivot)
        for t in range(p + 2, n):
            for q in range(2):
                mine = columns(t, c + 8 * q, 8)
                replaced(t, c + 8 * q, False)
                for m in range(8):
                    r, above, pivot_row = steps[8 * q + m]
                    f = mine[m] * r
                    for j in range(m + 1, 8):
                        mine[j] = mine[j] - f * above[8 * q + j]
                    for s in range(2):
                        rows[t][s] = rows[t][s] - f * pivot_row[s]
    return rows, pivots


def factor(a_ref, w_ref, g_ref):
    row = lax.broadcasted_iota(jnp.int32, (8, 128), 0)
    lane = lax.broadcasted_iota(jnp.int32, (8, 128), 1)
    width = a_ref.shape[0]
    for o in range(0, width, PANEL):
        end = o + PANEL
        rows = [[a_ref[o + 8 * t : o + 8 * t + 8, 128 * h : 128 * h + 128] for h in range(2)] for t in range(PANEL // 8)]
        rows, pivots = eliminate(rows, o)
        for t in range(PANEL // 8):
            scale = lax.rsqrt(pivots[t])
            for h in range(2):
                col = lane + 128 * h
                lower = col <= row + o + 8 * t
                g = rows[t][h] * scale
                w_ref[o + 8 * t : o + 8 * t + 8, 128 * h : 128 * h + 128] = jnp.where(lower, g, 0.0)
                g_ref[8 * t : 8 * t + 8, 128 * h : 128 * h + 128] = jnp.where(lower | (col >= end), g, 0.0)
        if end < width:
            g = g_ref[...]
            bounds = (end, end + PANEL, width) if end + PANEL < width else (end, width)
            for low, high in zip(bounds, bounds[1:]):
                first, last = low // 128 * 128, -(-high // 128) * 128
                update = row_dot(g[:, first:last], g, HIGHEST)[low - first : high - first]
                col = lax.broadcasted_iota(jnp.int32, (high - low, width), 1)
                a_ref[low:high, :] = jnp.where((col >= o) & (col < end), 0.0, a_ref[low:high, :]) - update


def solve_kernel(packed_ref, psi_ref, weights_ref, orbitals_ref, contribution_ref,
                 psi_v, out_v, a_ref, w_ref, r_ref, g_ref, in_sems, out_sems):
    rows, width = psi_ref.shape
    n = rows // PIECE
    ins = [
        pltpu.make_async_copy(psi_ref.at[pl.ds(c * PIECE, PIECE)], psi_v.at[pl.ds(c * PIECE, PIECE)], in_sems.at[c])
        for c in range(n)
    ]
    outs = [
        pltpu.make_async_copy(out_v.at[pl.ds(c * PIECE, PIECE)], orbitals_ref.at[pl.ds(c * PIECE, PIECE)], out_sems.at[c])
        for c in range(n)
    ]
    for copy in ins:
        copy.start()
    diagonals = [jnp.zeros((1, 128), F32) for _ in range(width // 128)]
    for i in range(width // 8):
        for h in range(width // 128):
            w_ref[8 * i : 8 * i + 8, 128 * h : 128 * h + 128] = packed_ref[17 * i + 8 * h : 17 * i + 8 * h + 8]
        diagonals[8 * i // 128] += packed_ref[17 * i + 16 : 17 * i + 17]
    packed = w_ref[...]
    turned = jnp.transpose(packed)
    row = lax.broadcasted_iota(jnp.int32, (width, width), 0)
    col = lax.broadcasted_iota(jnp.int32, (width, width), 1)
    diagonal = jnp.concatenate(diagonals, axis=1)
    a_ref[...] = jnp.where(row >= col, packed, turned)
    r_ref[...] = jnp.where(row < col, packed, jnp.where(row == col, jnp.broadcast_to(diagonal, packed.shape), turned))
    factor(a_ref, w_ref, g_ref)
    inverse = w_ref[...]
    half = jnp.dot(inverse, r_ref[...], precision=HIGHEST, preferred_element_type=F32)
    projected = lax.dot_general(half, inverse, (((1,), (1,)), ((), ())), precision=HIGHEST, preferred_element_type=F32)
    identity = jnp.where(row == col, 1.0, 0.0)
    rotation = row_dot(inverse, identity - step_size * projected, HIGHEST).astype(BF16)

    weights = weights_ref[...]
    on_diagonal = lax.broadcasted_iota(jnp.int32, (128, 128), 0) == lax.broadcasted_iota(jnp.int32, (128, 128), 1)
    parts = []
    for c in range(n):
        ins[c].wait()
        for s in range(PIECE // 256):
            start = c * PIECE + s * 256
            rotated = jnp.dot(psi_v[start : start + 256], rotation, preferred_element_type=F32)
            out_v[start : start + 256] = rotated.astype(BF16)
            weighted = rotated * rotated * weights
            weighted = weighted[:, :128] + weighted[:, 128:]
            for h in range(2):
                sums = jnp.sum(weighted[128 * h : 128 * h + 128], axis=1, keepdims=True)
                parts.append(jnp.sum(jnp.where(on_diagonal, sums, 0.0), axis=0, keepdims=True))
        outs[c].start()
    contribution = jnp.concatenate(parts, axis=0)
    for i in range(contribution_ref.shape[0]):
        contribution_ref[i] = contribution
    for copy in outs:
        copy.wait()


def in_vmem(x):
    return pltpu.with_memory_space_constraint(x, pltpu.VMEM)


def per_device(orbitals, potential, core_density, occupation, slice_counts):
    coefficient = (3.0 / jnp.pi) ** (1.0 / 3.0)
    rows, width = orbitals.shape
    peers = lax.axis_size(GRID)
    groups = lax.axis_size("cuts")
    blocks = rows // 128
    following = lax.ppermute(orbitals[:8], GRID, [((i + 1) % peers, i) for i in range(peers)])
    potential = potential.reshape(blocks, 128)
    packed, last, weights = pl.pallas_call(
        functools.partial(gram_kernel, width * groups),
        out_shape=(
            pltpu.VMEM((17 * width // 8, 128), F32),
            pltpu.VMEM((EDGE, width), BF16),
            pltpu.VMEM((1, width), F32),
        ),
        scratch_shapes=[pltpu.VMEM((rows, width), BF16)],
        name="gram",
    )(in_vmem(orbitals), potential, occupation.reshape(1, width), slice_counts.reshape(1, 1))
    chunk = 17 * 128
    packed = pl.pallas_call(border_kernel, out_shape=pltpu.VMEM((17 * width // 8, 128), F32), name="border")(
        in_vmem(packed), in_vmem(last), in_vmem(following)
    )
    mine = lax.all_to_all(packed.reshape(peers, 1, chunk), EXCHANGE, 0, 0, tiled=True)
    copies = pl.pallas_call(functools.partial(spread_kernel, rows * peers), out_shape=pltpu.VMEM((peers, 1, chunk), F32), name="spread")(in_vmem(mine))
    every = lax.all_to_all(copies, EXCHANGE, 0, 0, tiled=True)
    orbitals_out, contribution = pl.pallas_call(
        solve_kernel,
        out_shape=(
            jax.ShapeDtypeStruct((rows, width), BF16),
            pltpu.VMEM((groups, blocks, 128), F32),
        ),
        in_specs=[
            pl.BlockSpec(memory_space=pltpu.VMEM),
            pl.BlockSpec(memory_space=pl.ANY),
            pl.BlockSpec(memory_space=pltpu.VMEM),
        ],
        out_specs=(pl.BlockSpec(memory_space=pl.ANY), pl.BlockSpec(memory_space=pltpu.VMEM)),
        scratch_shapes=[
            pltpu.VMEM((rows, width), BF16),
            pltpu.VMEM((rows, width), BF16),
            pltpu.VMEM((width, width), F32),
            pltpu.VMEM((width, width), F32),
            pltpu.VMEM((width, width), F32),
            pltpu.VMEM((PANEL, width), F32),
            pltpu.SemaphoreType.DMA((rows // PIECE,)),
            pltpu.SemaphoreType.DMA((rows // PIECE,)),
        ],
        name="solve",
    )(in_vmem(every.reshape(17 * width // 8, 128)), orbitals, in_vmem(weights))
    density = core_density.reshape(blocks, 128) + lax.all_to_all(contribution, "cuts", 0, 0, tiled=True).sum(axis=0)
    potential_out = (1.0 - mixing) * potential + mixing * (-coefficient * jnp.cbrt(density))
    return (orbitals_out, potential_out.reshape(rows))


def solution(mesh):
    torus = Mesh(mesh.devices.reshape(mesh.shape["cuts"], 4, 4, 2), ("cuts", "z_hi", "z_lo", "x_lo"))
    in_specs = (P(GRID, "cuts"), P(GRID), P(GRID), P("cuts"), P("cuts"))
    out_specs = (P(GRID, "cuts"), P(GRID))
    return jax.shard_map(
        per_device, mesh=torus, in_specs=in_specs, out_specs=out_specs, check_vma=False
    )
```
